32 devices in a mesh: row: 16 (over z, y, core), col: 2 (over x).
Axes of the slice: x: 2, y: 2, z: 4, core: 2. Of those that a mesh axis runs over, the one named last changes fastest.
Arguments:
- spectral_field: float32 [2, 256, 256, 256], P(None, 'row', 'col'), may hold values from -4.5 to 4.5
Outputs:
- updated_field: float32 [2, 256, 256, 256], P(None, 'row', 'col')
- shell_spectrum: float32 [256], replicated
The draws below stay inside these ranges and needn't reach their ends.
All inputs are finite; a program needn't handle non-finite values.
Results may differ from the reference program's by a relative error of at most 0.0031.
Values may be sent and summed in bfloat16 or wider, within the bound.
A program may use at most 192 MiB of HBM per device.

```python
import math
import jax
import jax.numpy as jnp
from jax import lax

K = 256


def block_levels(key, dims, shards, smallest, top_value):
    factor_of = 1.0
    for axis_at, blocks in shards:
        draws = jax.random.uniform(jax.random.fold_in(jax.random.fold_in(key, 6), axis_at), (blocks,), jnp.float32, smallest / len(shards), top_value / len(shards))
        factor_of = factor_of * jnp.repeat(jnp.exp(draws), dims[axis_at] // blocks).reshape((-1,) + (1,) * (len(dims) - 1 - axis_at))
    return factor_of


def bell_draw(rng, shape, deviation, reach, cuts=(), kind=jnp.bfloat16):
    loudness = block_levels(rng, shape, cuts, -0.22, 0.18) if cuts else 1.0
    entries = jax.random.normal(rng, shape, jnp.float32) * deviation * loudness
    return jnp.minimum(jnp.maximum(entries, -reach), reach).astype(kind)


def setup_inputs(seed: int = 0) -> dict:
    splits = jax.random.split(jax.random.key(seed), 2)
    spectral_field = bell_draw(splits[0], (2, K, K, K), 0.7, 4.5, ((1, 16), (2, 2)), jnp.float32)
    return {"spectral_field": spectral_field}


phase_rate = 0.0002
coupling = 0.2

def wave_table(inputs, outputs, length, sine_sign, live_mask):
    phase_turns = jnp.mod(inputs[:, None] * outputs[None, :], length)
    phase_angle = phase_turns.astype(jnp.float32) * (2.0 * math.pi / length)
    live_rows = live_mask.astype(jnp.float32)[:, None]
    cosine_part = (jnp.cos(phase_angle) * live_rows).astype(jnp.bfloat16)
    sine_part = (sine_sign * jnp.sin(phase_angle) * live_rows).astype(jnp.bfloat16)
    return (cosine_part, sine_part)

def rotate(values_in, cosine_part, sine_part, einsum_form, factor):
    precise = lax.Precision.HIGHEST
    real_part = values_in[0].astype(jnp.float32)
    imag_part = values_in[1].astype(jnp.float32)
    cos_wide = cosine_part.astype(jnp.float32)
    sin_wide = sine_part.astype(jnp.float32)
    out_real = jnp.einsum(einsum_form, real_part, cos_wide, precision=precise) - jnp.einsum(einsum_form, imag_part, sin_wide, precision=precise)
    out_imag = jnp.einsum(einsum_form, real_part, sin_wide, precision=precise) + jnp.einsum(einsum_form, imag_part, cos_wide, precision=precise)
    return jnp.stack([out_real, out_imag]) * factor

def reference(spectral_field):
    mode_count = spectral_field.shape[1]
    grid_count = 2 * mode_count
    wavenumbers = jnp.arange(mode_count, dtype=jnp.int32) - mode_count // 2
    grid_points = jnp.arange(grid_count, dtype=jnp.int32)
    inv_cos, inv_sin = wave_table(wavenumbers, grid_points, grid_count, 1.0, jnp.ones((mode_count,), bool))
    fwd_cos, fwd_sin = wave_table(grid_points, wavenumbers, grid_count, -1.0, jnp.ones((grid_count,), bool))
    scale_in = 1.0 / math.sqrt(mode_count)
    scale_out = math.sqrt(mode_count) / grid_count
    coeffs = spectral_field.astype(jnp.bfloat16)
    along_z = rotate(coeffs, inv_cos, inv_sin, 'abc,cd->abd', scale_in).astype(jnp.bfloat16)
    along_y = rotate(along_z, inv_cos, inv_sin, 'abc,bd->adc', scale_in).astype(jnp.bfloat16)
    block_size = grid_count // 8
    pieces = []
    for number in range(8):
        z_block = lax.slice_in_dim(along_y, number * block_size, (number + 1) * block_size, axis=3)
        physical = rotate(z_block, inv_cos, inv_sin, 'abc,ad->dbc', scale_in)
        cubic_term = (coupling * (physical[0] * physical[0] + physical[1] * physical[1]) * physical).astype(jnp.bfloat16)
        pieces.append(rotate(cubic_term, fwd_cos, fwd_sin, 'abc,ad->dbc', scale_out).astype(jnp.bfloat16))
    back_x = jnp.concatenate(pieces, axis=3)
    back_y = rotate(back_x, fwd_cos, fwd_sin, 'abc,bd->adc', scale_out).astype(jnp.bfloat16)
    nonlinear = rotate(back_y, fwd_cos, fwd_sin, 'abc,cd->abd', scale_out)
    wave_first = wavenumbers[:, None, None]
    wave_second = wavenumbers[None, :, None]
    wave_third = wavenumbers[None, None, :]
    squared = wave_first * wave_first + wave_second * wave_second + wave_third * wave_third
    phase_angle = phase_rate * squared.astype(jnp.float32)
    cosine_part = jnp.cos(phase_angle)
    sine_part = jnp.sin(phase_angle)
    shifted_real = spectral_field[0] - nonlinear[1]
    shifted_imag = spectral_field[1] + nonlinear[0]
    new_real = shifted_real * cosine_part + shifted_imag * sine_part
    new_imag = shifted_imag * cosine_part - shifted_real * sine_part
    updated_field = jnp.stack([new_real, new_imag])
    energy = new_real * new_real + new_imag * new_imag
    shell_index = jnp.floor(jnp.sqrt(squared.astype(jnp.float32)) + 0.5).astype(jnp.int32)
    totals = jax.ops.segment_sum(energy.reshape(-1), shell_index.reshape(-1), num_segments=mode_count)
    counts = jax.ops.segment_sum(jnp.ones_like(energy).reshape(-1), shell_index.reshape(-1), num_segments=mode_count)
    shell_spectrum = totals / jnp.maximum(counts, 1.0)
    return (updated_field, shell_spectrum)
```

```python
import functools
import math

import jax
import jax.numpy as jnp
import ml_dtypes
import numpy as np
from jax import lax
from jax.experimental import pallas as pl
from jax.experimental.pallas import tpu as pltpu
from jax.sharding import PartitionSpec as P

phase_rate = 0.0002
coupling = 0.2
AXES = ("row", "col")
VMEM_LIMIT = 60 * 1024 * 1024


def base_tables(modes):
    grid = 2 * modes
    wave = np.arange(modes) - modes // 2
    turns = np.mod(wave[:, None] * np.arange(grid)[None, :], grid)
    angle = (turns.astype(np.float32) * np.float32(2.0 * math.pi / grid)).astype(np.float64)
    cosine = np.cos(angle).astype(np.float32)
    sine = np.sin(angle).astype(np.float32)
    return cosine, sine


def wide_table(modes):
    cosine, sine = base_tables(modes)
    return np.block([[cosine, sine], [-sine, cosine]]).astype(ml_dtypes.bfloat16)


def shell_counts(modes):
    wave = np.arange(modes, dtype=np.int64) - modes // 2
    squares = wave * wave
    pairs = np.bincount((squares[:, None] + squares[None, :]).ravel())
    total = np.zeros(len(pairs) + int(squares.max()), np.int64)
    for square in squares:
        total[square : square + len(pairs)] += pairs
    shell = np.floor(np.sqrt(np.arange(len(total), dtype=np.float64)) + 0.5).astype(np.int64)
    counts = np.bincount(shell, weights=total, minlength=modes)[:modes]
    return np.maximum(counts, 1.0).astype(np.float32)


def first_kernel(scale, field_ref, tall_ref, out_ref, wide_ref):
    width_x = field_ref.shape[1]
    grid = tall_ref.shape[0] // 2
    lanes = out_ref.shape[2]

    def pair(step, carry):
        x = 2 * step
        rows = []
        for k in range(2):
            rows.append(
                jnp.concatenate([field_ref[0, x + k], field_ref[1, x + k]], axis=1).astype(
                    jnp.bfloat16
                )
            )
        coeffs = jnp.concatenate(rows, axis=0)
        for part in range(2):
            product = (
                lax.dot_general(
                    tall_ref[part * grid : (part + 1) * grid, :],
                    coeffs,
                    (((1,), (1,)), ((), ())),
                    preferred_element_type=jnp.float32,
                )
                * scale
            )
            for k in range(2):
                wide_ref[pl.ds(part * width_x + x + k, grid, stride=2 * width_x), :] = product[
                    :, k * lanes : (k + 1) * lanes
                ]
        return carry

    lax.fori_loop(0, width_x // 2, pair, 0)
    group = out_ref.shape[0] // 16

    def narrow(step, carry):
        start = pl.multiple_of(step * group * width_x, group * width_x)
        block = wide_ref[pl.ds(start, group * width_x), :].astype(jnp.bfloat16)
        out_ref[pl.ds(step * group, group)] = block.reshape(group, width_x, lanes)
        return carry

    lax.fori_loop(0, 16, narrow, 0)


def middle_kernel(rows, cols, scale_in, scale_out, in_ref, wide_ref, tall_ref, out_ref):
    width_x, width_y = in_ref.shape[3], in_ref.shape[4]
    modes = rows * width_x
    grid = 2 * modes
    pieces = []
    for part in range(2):
        for col in range(cols):
            block = jnp.concatenate(
                [in_ref[row * cols + col, 0, part] for row in range(rows)], axis=0
            )
            pieces.append(block)
    lines = jnp.concatenate(pieces, axis=1)
    along_y = (
        jnp.dot(lines, wide_ref[...], preferred_element_type=jnp.float32) * scale_in
    ).astype(jnp.bfloat16)
    stacked = jnp.concatenate([along_y[:, :grid], along_y[:, grid:]], axis=0)
    step = grid // 2
    halves = []
    for start in range(0, grid, step):
        field = (
            jnp.dot(
                tall_ref[...], stacked[:, start : start + step], preferred_element_type=jnp.float32
            )
            * scale_in
        )
        real, imag = field[:grid], field[grid:]
        weight = coupling * (real * real + imag * imag)
        cubic = jnp.concatenate(
            [(weight * real).astype(jnp.bfloat16), (weight * imag).astype(jnp.bfloat16)], axis=0
        )
        halves.append(
            (
                jnp.dot(wide_ref[...], cubic, preferred_element_type=jnp.float32) * scale_out
            ).astype(jnp.bfloat16)
        )
    back = jnp.concatenate(
        [half[:modes] for half in halves] + [half[modes:] for half in halves], axis=1
    )
    back_y = (
        jnp.dot(back, tall_ref[...], preferred_element_type=jnp.float32) * scale_out
    ).astype(jnp.bfloat16)
    for part in range(2):
        for col in range(cols):
            start = part * modes + col * width_y
            for row in range(rows):
                out_ref[row * cols + col, 0, part] = back_y[
                    row * width_x : (row + 1) * width_x, start : start + width_y
                ]


def last_kernel(
    scale,
    nl_ref,
    field_ref,
    tall_ref,
    tri_ref,
    radius_ref,
    cos_xy_ref,
    sin_xy_ref,
    cos_z_ref,
    sin_z_ref,
    out_ref,
    total_ref,
    wide_ref,
):
    width_x, width_y, modes = field_ref.shape[1], field_ref.shape[2], field_ref.shape[3]
    grid = 2 * modes
    half = modes // 2
    group = nl_ref.shape[0] // 16

    def widen(step, carry):
        start = pl.multiple_of(step * group * width_x, group * width_x)
        block = nl_ref[pl.ds(step * group, group)].reshape(group * width_x, width_y)
        wide_ref[pl.ds(start, group * width_x), :] = block.astype(jnp.float32)
        return carry

    lax.fori_loop(0, 16, widen, 0)
    total_ref[...] = jnp.zeros_like(total_ref)
    cos_z, sin_z = cos_z_ref[...], sin_z_ref[...]
    shell_low = lax.broadcasted_iota(jnp.int32, (1, modes), 1).astype(jnp.float32)
    below = jnp.where(shell_low > 0.0, shell_low * shell_low - shell_low, -1.0)
    limits = [below, shell_low * shell_low + shell_low]

    def pair(step, carry):
        x = 2 * step
        columns = []
        for k in range(2):
            columns.append(
                jnp.concatenate(
                    [
                        wide_ref[pl.ds(part * width_x + x + k, grid, stride=2 * width_x), :]
                        for part in range(2)
                    ],
                    axis=0,
                ).astype(jnp.bfloat16)
            )
        lines = jnp.concatenate(columns, axis=1)
        nonlinear = (
            lax.dot_general(
                lines, tall_ref[...], (((0,), (0,)), ((), ())), preferred_element_type=jnp.float32
            )
            * scale
        )
        for k in range(2):
            block = nonlinear[k * width_y : (k + 1) * width_y]
            u = field_ref[0, x + k] - block[:, modes:]
            v = field_ref[1, x + k] + block[:, :modes]
            cos_xy, sin_xy = cos_xy_ref[x + k], sin_xy_ref[x + k]
            cosine = cos_xy * cos_z - sin_xy * sin_z
            sine = sin_xy * cos_z + cos_xy * sin_z
            new_real = u * cosine + v * sine
            new_imag = v * cosine - u * sine
            out_ref[0, x + k] = new_real
            out_ref[1, x + k] = new_imag
            energy = new_real * new_real + new_imag * new_imag
            high = energy.astype(jnp.bfloat16)
            rest = energy - high.astype(jnp.float32)
            middle = rest.astype(jnp.bfloat16)
            low = (rest - middle.astype(jnp.float32)).astype(jnp.bfloat16)
            running = jnp.zeros((width_y, half), jnp.float32)
            for piece in (low, middle, high):
                running += jnp.dot(piece, tri_ref[...], preferred_element_type=jnp.float32)
            radius = radius_ref[x + k]
            parts = []
            for start in range(0, modes, half):
                found = []
                for limit in limits:
                    room = limit[:, start : start + half] - radius
                    index = jnp.floor(jnp.sqrt(jnp.maximum(room, 0.0) + 0.5)).astype(jnp.int32)
                    index = jnp.minimum(index, half - 1)
                    value = jnp.take_along_axis(
                        running, index, axis=1, mode="promise_in_bounds"
                    )
                    found.append(jnp.where(room >= 0.0, value, 0.0))
                parts.append(found[1] - found[0])
            spread = jnp.concatenate(parts, axis=1)
            edge = radius + float(half * half)
            inside = (edge > limits[0]) & (edge <= limits[1])
            spread = spread + jnp.where(inside, energy[:, 0:1], 0.0)
            total_ref[...] += jnp.sum(spread, axis=0, keepdims=True)
        return carry

    lax.fori_loop(0, width_x // 2, pair, 0)


def whole(ndim):
    return pl.BlockSpec(memory_space=pltpu.VMEM)


def geometry(spectral_field):
    width_x, width_y, modes = spectral_field.shape[1:]
    half = modes // 2
    wave_x = lax.axis_index("row") * width_x + jnp.arange(width_x, dtype=jnp.int32) - half
    wave_y = lax.axis_index("col") * width_y + jnp.arange(width_y, dtype=jnp.int32) - half
    wave_z = jnp.arange(modes, dtype=jnp.int32) - half
    return wave_x * wave_x, wave_y * wave_y, wave_z * wave_z


def kernels_body(spectral_field):
    width_x, width_y, modes = spectral_field.shape[1:]
    rows, cols = lax.axis_size("row"), lax.axis_size("col")
    devices = rows * cols
    grid = 2 * modes
    planes = grid // devices
    half = modes // 2
    scale_in = 1.0 / math.sqrt(modes)
    scale_out = math.sqrt(modes) / grid
    table = wide_table(modes)
    wide = jnp.asarray(table)
    tall = jnp.asarray(np.ascontiguousarray(table.T))
    params = pltpu.CompilerParams(vmem_limit_bytes=VMEM_LIMIT)
    along_z = pl.pallas_call(
        functools.partial(first_kernel, scale_in),
        out_shape=jax.ShapeDtypeStruct((2 * grid, width_x, width_y), jnp.bfloat16),
        in_specs=[whole(4), whole(2)],
        out_specs=whole(3),
        scratch_shapes=[pltpu.VMEM((2 * grid * width_x, width_y), jnp.float32)],
        compiler_params=params,
        name="first",
    )(spectral_field, tall)
    along_z = along_z.reshape(devices, planes, 2, width_x, width_y)
    lines = lax.all_to_all(along_z, AXES, split_axis=0, concat_axis=0, tiled=True)
    block = pl.BlockSpec((devices, 1, 2, width_x, width_y), lambda z: (0, z, 0, 0, 0))
    back_y = pl.pallas_call(
        functools.partial(middle_kernel, rows, cols, scale_in, scale_out),
        grid=(planes,),
        out_shape=jax.ShapeDtypeStruct(lines.shape, jnp.bfloat16),
        in_specs=[
            block,
            pl.BlockSpec((grid, 2 * grid), lambda z: (0, 0)),
            pl.BlockSpec((2 * grid, grid), lambda z: (0, 0)),
        ],
        out_specs=block,
        compiler_params=params,
        name="middle",
    )(lines, wide, tall)
    home = lax.all_to_all(back_y, AXES, split_axis=0, concat_axis=0, tiled=True)
    home = home.reshape(2 * grid, width_x, width_y)
    square_x, square_y, square_z = geometry(spectral_field)
    radius = (square_x[:, None] + square_y[None, :]).astype(jnp.float32)[:, :, None]
    angle_xy = phase_rate * radius
    angle_z = phase_rate * square_z.astype(jnp.float32)[None, :]
    distance = np.abs(np.arange(modes) - half)
    triangle = (distance[:, None] <= np.arange(half)[None, :]).astype(ml_dtypes.bfloat16)
    updated_field, totals = pl.pallas_call(
        functools.partial(last_kernel, scale_out),
        out_shape=(
            jax.ShapeDtypeStruct(spectral_field.shape, jnp.float32),
            jax.ShapeDtypeStruct((1, modes), jnp.float32),
        ),
        in_specs=[whole(0)] * 9,
        out_specs=(whole(0), whole(0)),
        scratch_shapes=[pltpu.VMEM((2 * grid * width_x, width_y), jnp.float32)],
        compiler_params=params,
        name="last",
    )(
        home,
        spectral_field,
        tall,
        jnp.asarray(triangle),
        radius,
        jnp.cos(angle_xy),
        jnp.sin(angle_xy),
        jnp.cos(angle_z),
        jnp.sin(angle_z),
    )
    totals = lax.psum(totals[0], AXES)
    return updated_field, totals / jnp.asarray(shell_counts(modes))


def plain_body(spectral_field):
    width_x, width_y, modes = spectral_field.shape[1:]
    rows, cols = lax.axis_size("row"), lax.axis_size("col")
    devices = rows * cols
    grid = 2 * modes
    planes = grid // devices
    scale_in = 1.0 / math.sqrt(modes)
    scale_out = math.sqrt(modes) / grid
    table = jnp.asarray(wide_table(modes)).reshape(2, modes, 2, grid)

    def product(form, first, second, factor):
        out = jnp.einsum(form, first, second, preferred_element_type=jnp.float32)
        return out * factor

    coeffs = spectral_field.astype(jnp.bfloat16)
    along_z = product("pxyj,pjqn->nqxy", coeffs, table, scale_in).astype(jnp.bfloat16)
    lines = lax.all_to_all(along_z, AXES, split_axis=0, concat_axis=0, tiled=True)
    lines = lines.reshape(rows, cols, planes, 2, width_x, width_y)
    lines = lines.transpose(2, 3, 0, 4, 1, 5).reshape(planes, 2, modes, modes)
    along_y = product("zpxy,pyqn->zqxn", lines, table, scale_in).astype(jnp.bfloat16)
    field = product("zpxn,pxqm->zqmn", along_y, table, scale_in)
    real, imag = field[:, 0:1], field[:, 1:2]
    cubic = (coupling * (real * real + imag * imag) * field).astype(jnp.bfloat16)
    back_x = product("zqmn,pxqm->zpxn", cubic, table, scale_out).astype(jnp.bfloat16)
    back_y = product("zqxn,pyqn->zpxy", back_x, table, scale_out).astype(jnp.bfloat16)
    back_y = back_y.reshape(planes, 2, rows, width_x, cols, width_y)
    back_y = back_y.transpose(2, 4, 0, 1, 3, 5).reshape(grid, 2, width_x, width_y)
    home = lax.all_to_all(back_y, AXES, split_axis=0, concat_axis=0, tiled=True)
    nonlinear = product("nqxy,pjqn->pxyj", home, table, scale_out)
    square_x, square_y, square_z = geometry(spectral_field)
    squared = square_x[:, None, None] + square_y[None, :, None] + square_z[None, None, :]
    angle = phase_rate * squared.astype(jnp.float32)
    cosine, sine = jnp.cos(angle), jnp.sin(angle)
    u = spectral_field[0] - nonlinear[1]
    v = spectral_field[1] + nonlinear[0]
    new_real = u * cosine + v * sine
    new_imag = v * cosine - u * sine
    energy = new_real * new_real + new_imag * new_imag
    shell = jnp.floor(jnp.sqrt(squared.astype(jnp.float32)) + 0.5).astype(jnp.int32)
    bins = jnp.arange(modes, dtype=jnp.int32)

    def per_plane(plane):
        one_hot = (plane[1].reshape(-1)[:, None] == bins[None, :]).astype(jnp.float32)
        return jnp.dot(plane[0].reshape(-1), one_hot, precision=lax.Precision.HIGHEST)

    totals = lax.psum(jnp.sum(lax.map(per_plane, (energy, shell)), axis=0), AXES)
    return jnp.stack([new_real, new_imag]), totals / jnp.asarray(shell_counts(modes))


def body(spectral_field):
    width_x, width_y, modes = spectral_field.shape[1:]
    fits = width_x % 16 == 0 and width_y % 128 == 0 and (modes // 2) == 128
    return (kernels_body if fits else plain_body)(spectral_field)


def solution(mesh):
    in_specs = (P(None, "row", "col", None),)
    out_specs = (P(None, "row", "col", None), P())
    return jax.shard_map(body, mesh=mesh, in_specs=in_specs, out_specs=out_specs, check_vma=False)
```
